32 devices in a mesh: dap: 8 (over y, x, core), hc: 4 (over z).
Axes of the slice: x: 2, y: 2, z: 4, core: 2. Of those that a mesh axis runs over, the one named last changes fastest.
Arguments:
- alignment: bfloat16 [64, 512, 256], P('dap'), may hold values from -6 to 6
- align_mask: int32 [64, 512], P('dap'), may hold values 0 or 1
- residue_mask: int32 [512], replicated, may hold values 0 or 1
- chain_index: int32 [512], replicated, may hold values from 0 to 7, never falling along the last dimension, each value on 1 to 256 neighbouring positions
- pair_input: bfloat16 [512, 512, 128], P('dap', 'hc'), may hold values from -6 to 6
- offset_table: bfloat16 [66, 128], replicated, may hold values from -6 to 6
- bias_weight: bfloat16 [128, 8], replicated, may hold values from -16 to 16
- query_weight: bfloat16 [256, 256], P(None, 'hc'), may hold values from -0.375 to 0.375
- key_weight: bfloat16 [256, 256], P(None, 'hc'), may hold values from -0.375 to 0.375
- value_weight: bfloat16 [256, 256], P(None, 'hc'), may hold values from -0.375 to 0.375
- gate_weight: bfloat16 [256, 256], P(None, 'hc'), may hold values from -0.375 to 0.375
- output_weight: bfloat16 [256, 256], replicated, may hold values from -0.375 to 0.375
- left_gate_weight: bfloat16 [128, 128], replicated, may hold values from -0.5 to 0.5
- left_weight: bfloat16 [128, 128], replicated, may hold values from -0.5 to 0.5
- right_gate_weight: bfloat16 [128, 128], replicated, may hold values from -0.5 to 0.5
- right_weight: bfloat16 [128, 128], replicated, may hold values from -0.5 to 0.5
- update_gate_weight: bfloat16 [128, 128], replicated, may hold values from -0.5 to 0.5
- update_out_weight: bfloat16 [128, 128], replicated, may hold values from -0.5 to 0.5
Outputs:
- alignment_out: bfloat16 [64, 512, 256], P('dap')
- pair_out: bfloat16 [512, 512, 128], P('dap', 'hc')
The draws below stay inside these ranges and needn't reach their ends.
All inputs are finite; a program needn't handle non-finite values. No bound on the sum of `align_mask` on one device may be relied on, other than what follows from the above.
Results may differ from the reference program's by a relative error of at most 0.0079.
Values may be sent and summed in bfloat16 or wider, within the bound.
A program may use at most 128 MiB of HBM per device.

```python
import math
import jax
import jax.numpy as jnp
import numpy as np
from jax import lax

C_M = 256
C_Z = 128
C_TRI = 128
HEADS = 8
HEAD_DIM = 32
REACH = 32
CHAINS = 8
RESIDUES = 512
SEQUENCES = 64


def draw_bias_weight(key, part):
    initial = jnp.clip(jax.random.normal(key, (C_Z, HEADS), jnp.float32), -4.0, 4.0) / math.sqrt(C_Z)
    return initial.astype(jnp.bfloat16)


def plant(result, own_key, least, high):
    shape = result.shape
    spot = [jax.random.randint(jax.random.fold_in(own_key, axis), (), 0, shape[axis]) for axis in range(len(shape))]
    result = result.at[tuple(spot)].set(least)
    longest = shape.index(max(shape))
    spot[longest] = (spot[longest] + 1) % shape[longest]
    return result.at[tuple(spot)].set(high)


def block_levels(rng, extent, cuts, smallest, largest):
    loudness, own = 1.0, jax.random.fold_in(rng, 6)
    for dim, blocks in cuts:
        steps = jnp.exp(jax.random.uniform(jax.random.fold_in(own, dim), (blocks,), jnp.float32, smallest / len(cuts), largest / len(cuts)))
        loudness = loudness * jnp.repeat(steps, extent[dim] // blocks).reshape([-1 if axis == dim else 1 for axis in range(len(extent))])
    return loudness


def length_profile(count, total, limit, slope):
    loads = [(1 << 20) // math.isqrt(standing ** slope) + 1 for standing in range(2, count + 1)]
    surplus, given = total - limit - (count - 1), [1] * (count - 1)
    while surplus > 0:
        candidates = [i for i in range(count - 1) if given[i] < limit]
        mass, left = sum([loads[i] for i in candidates]), surplus
        for i in candidates:
            extra = min(limit - given[i], max(1, left * loads[i] // mass), surplus)
            given[i] = given[i] + extra
            surplus = surplus - extra
    return np.array([limit] + given)


def uneven_parts(rng, count, total, limit, lean):
    if count == 2:
        one = jax.random.randint(rng, (), max(1, total - limit), min(limit, total - 1) + 1)
        return jnp.stack([one, total - one])
    tallies = jnp.asarray(length_profile(count, total, limit, lean), jnp.int32)
    twos = (count - 1) // 2
    giver, receiver = tallies[1:1 + 2 * twos:2], tallies[2:2 + 2 * twos:2]
    margin = jnp.minimum(giver - 1, limit - receiver)
    shifted = jax.random.randint(jax.random.fold_in(rng, 1), (twos,), 0, 1 << 20) % (margin + 1)
    tallies = tallies.at[1:1 + 2 * twos:2].set(giver - shifted).at[2:2 + 2 * twos:2].set(receiver + shifted)
    return tallies[jax.random.permutation(jax.random.fold_in(rng, 2), count)]


def gaussian(stream_key, dims, width, limit, cuts=(), held_as=jnp.bfloat16):
    drawn = jax.random.normal(stream_key, dims, jnp.float32) * width
    if len(cuts) > 0:
        drawn = block_levels(stream_key, dims, cuts, -0.22, 0.18) * drawn
    return jnp.clip(drawn, min=-limit, max=limit).astype(held_as)


def setup_inputs(seed: int = 0) -> dict:
    seeds = jax.random.split(jax.random.key(seed), 19)
    alignment = gaussian(seeds[0], (SEQUENCES, RESIDUES, C_M), 1.0, 6.0, ((0, 8),))
    align_mask = plant((jax.random.randint(seeds[1], (SEQUENCES, RESIDUES), 0, 8) < 7).astype(jnp.int32), jax.random.fold_in(seeds[1], 1), 0, 1)
    residue_mask = plant((jax.random.randint(seeds[2], (RESIDUES,), 0, 16) < 15).astype(jnp.int32), jax.random.fold_in(seeds[2], 1), 0, 1)
    chain_index = jnp.searchsorted(jnp.cumsum(uneven_parts(seeds[3], CHAINS, RESIDUES, RESIDUES // 2, 0)), jnp.arange(RESIDUES), side="right").astype(jnp.int32)
    pair_input = gaussian(seeds[4], (RESIDUES, RESIDUES, C_Z), 1.0, 6.0, ((0, 8), (1, 4)))
    offset_table = gaussian(seeds[5], (2 * REACH + 2, C_Z), 1.0, 6.0)
    bias_weight = draw_bias_weight(jax.random.fold_in(seeds[18], 71), 0)
    query_weight = gaussian(seeds[7], (C_M, HEADS * HEAD_DIM), C_M ** -0.5, 0.375, ((1, 4),))
    key_weight = gaussian(seeds[8], (C_M, HEADS * HEAD_DIM), C_M ** -0.5, 0.375, ((1, 4),))
    value_weight = gaussian(seeds[9], (C_M, HEADS * HEAD_DIM), C_M ** -0.5, 0.375, ((1, 4),))
    gate_weight = gaussian(seeds[10], (C_M, HEADS * HEAD_DIM), C_M ** -0.5, 0.375, ((1, 4),))
    output_weight = gaussian(seeds[11], (HEADS * HEAD_DIM, C_M), (HEADS * HEAD_DIM) ** -0.5, 0.375)
    left_gate_weight = gaussian(seeds[12], (C_Z, C_TRI), C_Z ** -0.5, 0.5)
    left_weight = gaussian(seeds[13], (C_Z, C_TRI), C_Z ** -0.5, 0.5)
    right_gate_weight = gaussian(seeds[14], (C_Z, C_TRI), C_Z ** -0.5, 0.5)
    right_weight = gaussian(seeds[15], (C_Z, C_TRI), C_Z ** -0.5, 0.5)
    update_gate_weight = gaussian(seeds[16], (C_Z, C_Z), C_Z ** -0.5, 0.5)
    update_out_weight = gaussian(seeds[17], (C_TRI, C_Z), C_TRI ** -0.5, 0.5)
    return {"alignment": alignment, "align_mask": align_mask, "residue_mask": residue_mask, "chain_index": chain_index, "pair_input": pair_input, "offset_table": offset_table, "bias_weight": bias_weight, "query_weight": query_weight, "key_weight": key_weight, "value_weight": value_weight, "gate_weight": gate_weight, "output_weight": output_weight, "left_gate_weight": left_gate_weight, "left_weight": left_weight, "right_gate_weight": right_gate_weight, "right_weight": right_weight, "update_gate_weight": update_gate_weight, "update_out_weight": update_out_weight}


EPSILON = 1e-05
MASKED = 1000000000.0

def normalize(values, along):
    values = values.astype(jnp.float32)
    average = lax.optimization_barrier(jnp.mean(values, axis=along, keepdims=True))
    centred = values - average
    variance = lax.optimization_barrier(jnp.mean(centred * centred, axis=along, keepdims=True))
    return centred * lax.rsqrt(variance + EPSILON)

def reference(alignment, align_mask, residue_mask, chain_index, pair_input, offset_table, bias_weight, query_weight, key_weight, value_weight, gate_weight, output_weight, left_gate_weight, left_weight, right_gate_weight, right_weight, update_gate_weight, update_out_weight):
    positions = jnp.arange(RESIDUES, dtype=jnp.int32)
    offsets = jnp.clip(positions[:, None] - positions[None, :] + REACH, 0, 2 * REACH)
    bin_index = jnp.where(chain_index[:, None] == chain_index[None, :], offsets, 2 * REACH + 1).astype(jnp.int32)
    pair_state = pair_input.astype(jnp.float32) + offset_table.astype(jnp.float32)[bin_index]
    pair_norm = normalize(pair_state, 2).astype(jnp.bfloat16)
    head_bias = jnp.einsum('ijc,ch->hij', pair_norm.astype(jnp.float32), bias_weight.astype(jnp.float32))
    align_norm = normalize(alignment, 2).astype(jnp.bfloat16)
    key_bias = MASKED * ((align_mask * residue_mask[None, :]).astype(jnp.float32) - 1.0)
    scaling = HEAD_DIM ** (-0.5)

    def per_sequence(members):
        sequence_rows, masking = members
        query_seq = (jnp.dot(sequence_rows, query_weight, preferred_element_type=jnp.float32) * scaling).astype(jnp.bfloat16)
        keys_seq = jnp.dot(sequence_rows, key_weight, preferred_element_type=jnp.float32).astype(jnp.bfloat16)
        values_seq = jnp.dot(sequence_rows, value_weight, preferred_element_type=jnp.float32).astype(jnp.bfloat16)
        gates_seq = jnp.dot(sequence_rows, gate_weight, preferred_element_type=jnp.float32).astype(jnp.bfloat16)
        query_seq = query_seq.reshape(RESIDUES, HEADS, HEAD_DIM).astype(jnp.float32)
        keys_seq = keys_seq.reshape(RESIDUES, HEADS, HEAD_DIM).astype(jnp.float32)
        values_seq = values_seq.reshape(RESIDUES, HEADS, HEAD_DIM).astype(jnp.float32)
        gates_seq = gates_seq.reshape(RESIDUES, HEADS, HEAD_DIM).astype(jnp.float32)
        scores = jnp.einsum('ihd,jhd->hij', query_seq, keys_seq) + head_bias + masking[None, None, :]
        weights = jax.nn.softmax(scores, axis=-1).astype(jnp.bfloat16)
        mixed = jnp.einsum('hij,jhd->ihd', weights.astype(jnp.float32), values_seq)
        mixed = (mixed * jax.nn.sigmoid(gates_seq)).astype(jnp.bfloat16)
        mixed = mixed.reshape(RESIDUES, HEADS * HEAD_DIM)
        return jnp.dot(mixed, output_weight, preferred_element_type=jnp.float32)
    merged = lax.map(per_sequence, (align_norm, key_bias))
    alignment_out = (alignment.astype(jnp.float32) + merged).astype(jnp.bfloat16)
    pair_mask = (residue_mask[:, None] * residue_mask[None, :]).astype(jnp.float32)
    norm_wide = pair_norm.astype(jnp.float32)

    def edge(gate_matrix, proj_matrix):
        gated = jax.nn.sigmoid(jnp.einsum('ikc,ce->eik', norm_wide, gate_matrix.astype(jnp.float32)))
        projected = jnp.einsum('ikc,ce->eik', norm_wide, proj_matrix.astype(jnp.float32))
        return (gated * projected * pair_mask[None, :, :]).astype(jnp.bfloat16)
    left_side = edge(left_gate_weight, left_weight)
    right_side = edge(right_gate_weight, right_weight)

    def per_channel(channel_pair):
        return jnp.dot(channel_pair[0], channel_pair[1].T, preferred_element_type=jnp.float32).astype(jnp.bfloat16)
    triangle = lax.map(per_channel, (left_side, right_side))
    triangle_norm = normalize(triangle, 0).astype(jnp.bfloat16)
    update_gate = jax.nn.sigmoid(jnp.einsum('ijc,ce->ije', norm_wide, update_gate_weight.astype(jnp.float32)))
    update = jnp.einsum('eij,ec->ijc', triangle_norm.astype(jnp.float32), update_out_weight.astype(jnp.float32)) * update_gate
    pair_out = (pair_state + update).astype(jnp.bfloat16)
    return (alignment_out, pair_out)
```

```python
import jax
import jax.numpy as jnp
from jax import lax
from jax.experimental import pallas as pl
from jax.experimental.pallas import tpu as pltpu
from jax.sharding import PartitionSpec as P

HEAD_DIM = 32
REACH = 32


EPSILON = 1e-05
MASKED = 1000000000.0


def normalize(values, along):
    values = values.astype(jnp.float32)
    average = jnp.mean(values, axis=along, keepdims=True)
    centred = values - average
    variance = jnp.mean(centred * centred, axis=along, keepdims=True)
    return centred * lax.rsqrt(variance + EPSILON)


def project(inputs, weight, pattern):
    return jnp.einsum(pattern, inputs, weight, preferred_element_type=jnp.float32)


def attention_kernel(tile, query_ref, key_ref, value_ref, gate_ref, mask_ref, bias_ref, out_ref):
    width, residues = query_ref.shape[1:]
    keys = key_ref[0]
    masking = mask_ref[0]
    rows = lax.broadcasted_iota(jnp.int32, (width, tile), 0)
    for head in range(width // HEAD_DIM):
        own = slice(head * HEAD_DIM, (head + 1) * HEAD_DIM)
        for first in range(0, residues, tile):
            span = slice(first, first + tile)
            query = query_ref[0, :, span]
            query = jnp.where((rows >= own.start) & (rows < own.stop), query, jnp.zeros_like(query))
            scores = jnp.dot(keys, query, preferred_element_type=jnp.float32)
            scores = scores + bias_ref[head, :, span] + masking
            top = jnp.max(scores, axis=0, keepdims=True)
            weights = jnp.exp(scores - top)
            total = jnp.sum(weights, axis=0, keepdims=True)
            mixed = jnp.dot(
                value_ref[0, own, :], weights.astype(jnp.bfloat16), preferred_element_type=jnp.float32
            )
            gate = jax.nn.sigmoid(gate_ref[0, own, span].astype(jnp.float32))
            out_ref[0, own, span] = (mixed / total * gate).astype(jnp.bfloat16)


def attention(queries, keys, values, gates, masking, bias):
    count, width, residues = queries.shape
    tile = min(256, residues)
    wide = pl.BlockSpec((1, width, residues), lambda s: (s, 0, 0))
    return pl.pallas_call(
        lambda *refs: attention_kernel(tile, *refs),
        name="attention",
        grid=(count,),
        in_specs=[
            wide,
            pl.BlockSpec((1, residues, width), lambda s: (s, 0, 0)),
            wide,
            wide,
            pl.BlockSpec((1, residues, 1), lambda s: (s, 0, 0)),
            pl.BlockSpec(bias.shape, lambda s: (0, 0, 0)),
        ],
        out_specs=wide,
        out_shape=jax.ShapeDtypeStruct(queries.shape, jnp.bfloat16),
        cost_estimate=pl.CostEstimate(
            flops=32 * count * width * residues * residues,
            bytes_accessed=10 * count * width * residues + 4 * bias.size,
            transcendentals=count * bias.size,
        ),
    )(queries, keys, values, gates, masking, bias)


def triangle_kernel(left_ref, right_ref, out_ref):
    dap_size, hc_size, _, row_count, col_count = left_ref.shape

    def joined(ref):
        parts = [ref[:, h, 0].reshape(dap_size * row_count, col_count) for h in range(hc_size)]
        return jnp.concatenate(parts, axis=1)

    product = lax.dot_general(
        joined(left_ref), joined(right_ref), (((1,), (1,)), ((), ())), preferred_element_type=jnp.float32
    ).astype(jnp.bfloat16)
    for a in range(dap_size):
        for h in range(hc_size):
            out_ref[a, h, 0] = product[
                a * row_count : (a + 1) * row_count, h * col_count : (h + 1) * col_count
            ]


def triangle_product(left, right):
    dap_size, hc_size, channels, row_count, col_count = left.shape
    spec = pl.BlockSpec((dap_size, hc_size, 1, row_count, col_count), lambda c: (0, 0, c, 0, 0))
    return pl.pallas_call(
        triangle_kernel,
        name="triangle",
        grid=(channels,),
        in_specs=[spec, spec],
        out_specs=spec,
        out_shape=jax.ShapeDtypeStruct(left.shape, jnp.bfloat16),
        cost_estimate=pl.CostEstimate(
            flops=4 * left.size * dap_size * row_count, bytes_accessed=6 * left.size, transcendentals=0
        ),
    )(left, right)


def exchange(blocks):
    return lax.all_to_all(blocks, ("dap", "hc"), split_axis=0, concat_axis=0, tiled=True)


def on_device(
    alignment,
    align_mask,
    residue_mask,
    chain_index,
    pair_input,
    offset_table,
    bias_weight,
    query_weight,
    key_weight,
    value_weight,
    gate_weight,
    output_weight,
    left_gate_weight,
    left_weight,
    right_gate_weight,
    right_weight,
    update_gate_weight,
    update_out_weight,
):
    row_count = pair_input.shape[0]
    col_count = pair_input.shape[1]
    residues = residue_mask.shape[0]
    dap_size = lax.axis_size("dap")
    hc_size = lax.axis_size("hc")
    row_first = lax.axis_index("dap") * row_count
    col_first = lax.axis_index("hc") * col_count
    row_ids = row_first + jnp.arange(row_count, dtype=jnp.int32)
    col_ids = col_first + jnp.arange(col_count, dtype=jnp.int32)
    row_chain = lax.dynamic_slice_in_dim(chain_index, row_first, row_count, 0)
    col_chain = lax.dynamic_slice_in_dim(chain_index, col_first, col_count, 0)
    offsets = jnp.clip(row_ids[:, None] - col_ids[None, :] + REACH, 0, 2 * REACH)
    bin_index = jnp.where(row_chain[:, None] == col_chain[None, :], offsets, 2 * REACH + 1)
    slot_count = 128
    one_hot = (
        bin_index[:, :, None] == jnp.arange(slot_count, dtype=jnp.int32)[None, None, :]
    ).astype(jnp.bfloat16)
    padded_table = jnp.pad(offset_table, ((0, slot_count - offset_table.shape[0]), (0, 0)))
    pair_state = pair_input.astype(jnp.float32) + project(one_hot, padded_table, "ijb,bc->ijc")
    pair_norm = normalize(pair_state, 2).astype(jnp.bfloat16)
    head_bias = project(pair_norm, bias_weight, "ijc,ch->ihj")
    head_bias = lax.all_to_all(head_bias, "hc", split_axis=1, concat_axis=2, tiled=True)
    align_norm = normalize(alignment, 2).astype(jnp.bfloat16)
    scaling = HEAD_DIM ** (-0.5)
    queries = (project(align_norm, query_weight, "snc,ce->sen") * scaling).astype(jnp.bfloat16)
    keys_all = project(align_norm, key_weight, "snc,ce->sne").astype(jnp.bfloat16)
    values_all = project(align_norm, value_weight, "snc,ce->sen").astype(jnp.bfloat16)
    gates_all = project(align_norm, gate_weight, "snc,ce->sen").astype(jnp.bfloat16)
    key_bias = MASKED * ((align_mask * residue_mask[None, :]).astype(jnp.float32) - 1.0)
    bias_rows = lax.all_gather(head_bias, "dap", axis=0, tiled=True)
    residue_rows = lax.dynamic_slice_in_dim(residue_mask, row_first, row_count, 0)
    residue_cols = lax.dynamic_slice_in_dim(residue_mask, col_first, col_count, 0)
    pair_mask = (residue_rows[:, None] * residue_cols[None, :]).astype(jnp.float32)
    update_gate = jax.nn.sigmoid(project(pair_norm, update_gate_weight, "ijc,ce->ije"))
    left_side = jax.nn.sigmoid(project(pair_norm, left_gate_weight, "ijc,ce->eij")) * project(
        pair_norm, left_weight, "ijc,ce->eij"
    )
    left_side = (left_side * pair_mask[None, :, :]).astype(jnp.bfloat16)
    right_side = jax.nn.sigmoid(project(pair_norm, right_gate_weight, "ijc,ce->eij")) * project(
        pair_norm, right_weight, "ijc,ce->eij"
    )
    right_side = (right_side * pair_mask[None, :, :]).astype(jnp.bfloat16)
    own_channels = left_side.shape[0] // (dap_size * hc_size)
    shares = (dap_size, hc_size, own_channels, row_count, col_count)
    right_all = exchange(right_side).reshape(shares)
    left_side, bias_rows = lax.optimization_barrier((left_side, bias_rows))
    left_all = exchange(left_side).reshape(shares)
    bias_heads = jnp.transpose(bias_rows, (1, 2, 0))
    attended = attention(queries, keys_all, values_all, gates_all, key_bias[:, :, None], bias_heads)
    triangle = triangle_product(left_all, right_all)
    triangle, attended = lax.optimization_barrier((triangle, attended))
    triangle_local = exchange(triangle.reshape(left_side.shape))
    merged = project(
        lax.all_gather(attended, "hc", axis=1, tiled=True), output_weight, "sen,ec->snc"
    )
    alignment_out = (alignment.astype(jnp.float32) + merged).astype(jnp.bfloat16)
    triangle_norm = normalize(triangle_local, 0).astype(jnp.bfloat16)
    update = project(triangle_norm, update_out_weight, "eij,ec->ijc") * update_gate
    pair_out = (pair_state + update).astype(jnp.bfloat16)
    return (alignment_out, pair_out)


def solution(mesh):
    placed = (
        P("dap", None, None),
        P("dap", None),
        P(),
        P(),
        P("dap", "hc", None),
        P(),
        P(),
        P(None, "hc"),
        P(None, "hc"),
        P(None, "hc"),
        P(None, "hc"),
        P(),
        P(),
        P(),
        P(),
        P(),
        P(),
        P(),
    )
    return jax.shard_map(
        on_device,
        mesh=mesh,
        in_specs=placed,
        out_specs=(P("dap", None, None), P("dap", "hc", None)),
        check_vma=False,
    )
```

```python
import jax
import jax.numpy as jnp
from jax import lax
from jax.experimental import pallas as pl
from jax.experimental.pallas import tpu as pltpu
from jax.sharding import PartitionSpec as P

HEAD_DIM = 32
REACH = 32


EPSILON = 1e-05
MASKED = 1000000000.0


def normalize(values, along):
    values = values.astype(jnp.float32)
    average = jnp.mean(values, axis=along, keepdims=True)
    centred = values - average
    variance = jnp.mean(centred * centred, axis=along, keepdims=True)
    return centred * lax.rsqrt(variance + EPSILON)


def project(inputs, weight, pattern):
    return jnp.einsum(pattern, inputs, weight, preferred_element_type=jnp.float32)


def attention_kernel(tile, query_ref, key_ref, value_ref, gate_ref, mask_ref, bias_ref, out_ref):
    width, residues = query_ref.shape[1:]
    keys = key_ref[0]
    masking = mask_ref[0]
    rows = lax.broadcasted_iota(jnp.int32, (width, tile), 0)
    for head in range(width // HEAD_DIM):
        own = slice(head * HEAD_DIM, (head + 1) * HEAD_DIM)
        for first in range(0, residues, tile):
            span = slice(first, first + tile)
            query = query_ref[0, :, span]
            query = jnp.where((rows >= own.start) & (rows < own.stop), query, jnp.zeros_like(query))
            scores = jnp.dot(keys, query, preferred_element_type=jnp.float32)
            scores = scores + bias_ref[head, :, span] + masking
            top = jnp.max(scores, axis=0, keepdims=True)
            weights = jnp.exp(scores - top)
            total = jnp.sum(weights, axis=0, keepdims=True)
            mixed = jnp.dot(
                value_ref[0, own, :], weights.astype(jnp.bfloat16), preferred_element_type=jnp.float32
            )
            gate = jax.nn.sigmoid(gate_ref[0, own, span].astype(jnp.float32))
            out_ref[0, own, span] = (mixed / total * gate).astype(jnp.bfloat16)


def attention(queries, keys, values, gates, masking, bias):
    count, width, residues = queries.shape
    tile = min(256, residues)
    wide = pl.BlockSpec((1, width, residues), lambda s: (s, 0, 0))
    return pl.pallas_call(
        lambda *refs: attention_kernel(tile, *refs),
        name="attention",
        grid=(count,),
        in_specs=[
            wide,
            pl.BlockSpec((1, residues, width), lambda s: (s, 0, 0)),
            wide,
            wide,
            pl.BlockSpec((1, residues, 1), lambda s: (s, 0, 0)),
            pl.BlockSpec(bias.shape, lambda s: (0, 0, 0)),
        ],
        out_specs=wide,
        out_shape=jax.ShapeDtypeStruct(queries.shape, jnp.bfloat16),
        cost_estimate=pl.CostEstimate(
            flops=32 * count * width * residues * residues,
            bytes_accessed=10 * count * width * residues + 4 * bias.size,
            transcendentals=count * bias.size,
        ),
    )(queries, keys, values, gates, masking, bias)


def triangle_kernel(left_ref, right_ref, out_ref):
    dap_size, hc_size, _, row_count, col_count = left_ref.shape

    def joined(ref):
        parts = [ref[:, h, 0].reshape(dap_size * row_count, col_count) for h in range(hc_size)]
        return jnp.concatenate(parts, axis=1)

    product = lax.dot_general(
        joined(left_ref), joined(right_ref), (((1,), (1,)), ((), ())), preferred_element_type=jnp.float32
    ).astype(jnp.bfloat16)
    for a in range(dap_size):
        for h in range(hc_size):
            out_ref[a, h, 0] = product[
                a * row_count : (a + 1) * row_count, h * col_count : (h + 1) * col_count
            ]


def triangle_product(left, right):
    dap_size, hc_size, channels, row_count, col_count = left.shape
    spec = pl.BlockSpec((dap_size, hc_size, 1, row_count, col_count), lambda c: (0, 0, c, 0, 0))
    return pl.pallas_call(
        triangle_kernel,
        name="triangle",
        grid=(channels,),
        in_specs=[spec, spec],
        out_specs=spec,
        out_shape=jax.ShapeDtypeStruct(left.shape, jnp.bfloat16),
        cost_estimate=pl.CostEstimate(
            flops=4 * left.size * dap_size * row_count, bytes_accessed=6 * left.size, transcendentals=0
        ),
    )(left, right)


def exchange(blocks):
    return lax.all_to_all(blocks, ("dap", "hc"), split_axis=0, concat_axis=0, tiled=True)


def line_steps(early, step):
    size = lax.axis_size("hc")
    up = [(i, i + 1) for i in range(step - 1, size - 1)]
    down = [(i + 1, i) for i in range(size - step)]
    return lax.ppermute(early[0], "hc", up), lax.ppermute(early[1], "hc", down)


def line_gather(block, first, weight):
    size = lax.axis_size("hc")
    here = lax.axis_index("hc")
    width = block.shape[1]
    passed = [(block, block), first]
    for step in range(2, size):
        passed.append(line_steps(passed[-1], step))
    pieces = [block] + [passed[step][0] + passed[size - step][1] for step in range(1, size)]
    rows = [
        lax.dynamic_slice_in_dim(weight, lax.rem(here - step + size, size) * width, width, 0)
        for step in range(size)
    ]
    return jnp.concatenate(pieces, axis=1), jnp.concatenate(rows, axis=0)


def on_device(
    alignment,
    align_mask,
    residue_mask,
    chain_index,
    pair_input,
    offset_table,
    bias_weight,
    query_weight,
    key_weight,
    value_weight,
    gate_weight,
    output_weight,
    left_gate_weight,
    left_weight,
    right_gate_weight,
    right_weight,
    update_gate_weight,
    update_out_weight,
):
    row_count = pair_input.shape[0]
    col_count = pair_input.shape[1]
    residues = residue_mask.shape[0]
    dap_size = lax.axis_size("dap")
    hc_size = lax.axis_size("hc")
    row_first = lax.axis_index("dap") * row_count
    col_first = lax.axis_index("hc") * col_count
    row_ids = row_first + jnp.arange(row_count, dtype=jnp.int32)
    col_ids = col_first + jnp.arange(col_count, dtype=jnp.int32)
    row_chain = lax.dynamic_slice_in_dim(chain_index, row_first, row_count, 0)
    col_chain = lax.dynamic_slice_in_dim(chain_index, col_first, col_count, 0)
    offsets = jnp.clip(row_ids[:, None] - col_ids[None, :] + REACH, 0, 2 * REACH)
    bin_index = jnp.where(row_chain[:, None] == col_chain[None, :], offsets, 2 * REACH + 1)
    slot_count = 128
    one_hot = (
        bin_index[:, :, None] == jnp.arange(slot_count, dtype=jnp.int32)[None, None, :]
    ).astype(jnp.bfloat16)
    padded_table = jnp.pad(offset_table, ((0, slot_count - offset_table.shape[0]), (0, 0)))
    pair_state = pair_input.astype(jnp.float32) + project(one_hot, padded_table, "ijb,bc->ijc")
    pair_norm = normalize(pair_state, 2).astype(jnp.bfloat16)
    head_bias = project(pair_norm, bias_weight, "ijc,ch->ihj")
    head_bias = lax.all_to_all(head_bias, "hc", split_axis=1, concat_axis=2, tiled=True)
    align_norm = normalize(alignment, 2).astype(jnp.bfloat16)
    scaling = HEAD_DIM ** (-0.5)
    queries = (project(align_norm, query_weight, "snc,ce->sen") * scaling).astype(jnp.bfloat16)
    keys_all = project(align_norm, key_weight, "snc,ce->sne").astype(jnp.bfloat16)
    values_all = project(align_norm, value_weight, "snc,ce->sen").astype(jnp.bfloat16)
    gates_all = project(align_norm, gate_weight, "snc,ce->sen").astype(jnp.bfloat16)
    key_bias = MASKED * ((align_mask * residue_mask[None, :]).astype(jnp.float32) - 1.0)
    bias_rows = lax.all_gather(head_bias, "dap", axis=0, tiled=True)
    residue_rows = lax.dynamic_slice_in_dim(residue_mask, row_first, row_count, 0)
    residue_cols = lax.dynamic_slice_in_dim(residue_mask, col_first, col_count, 0)
    pair_mask = (residue_rows[:, None] * residue_cols[None, :]).astype(jnp.float32)
    update_gate = jax.nn.sigmoid(project(pair_norm, update_gate_weight, "ijc,ce->ije"))
    left_side = jax.nn.sigmoid(project(pair_norm, left_gate_weight, "ijc,ce->eij")) * project(
        pair_norm, left_weight, "ijc,ce->eij"
    )
    left_side = (left_side * pair_mask[None, :, :]).astype(jnp.bfloat16)
    right_side = jax.nn.sigmoid(project(pair_norm, right_gate_weight, "ijc,ce->eij")) * project(
        pair_norm, right_weight, "ijc,ce->eij"
    )
    right_side = (right_side * pair_mask[None, :, :]).astype(jnp.bfloat16)
    own_channels = left_side.shape[0] // (dap_size * hc_size)
    shares = (dap_size, hc_size, own_channels, row_count, col_count)
    left_all = exchange(left_side).reshape(shares)
    right_side, bias_rows, left_all = lax.optimization_barrier((right_side, bias_rows, left_all))
    right_all = exchange(right_side).reshape(shares)
    bias_heads = jnp.transpose(bias_rows, (1, 2, 0))
    attended = attention(queries, keys_all, values_all, gates_all, key_bias[:, :, None], bias_heads)
    first = line_steps((attended, attended), 1)
    right_all, first = lax.optimization_barrier((right_all, first))
    triangle = triangle_product(left_all, right_all)
    triangle, attended = lax.optimization_barrier((triangle, attended))
    triangle_local = exchange(triangle.reshape(left_side.shape))
    pieces, weight = line_gather(attended, first, output_weight)
    merged = project(pieces, weight, "sen,ec->snc")
    alignment_out = (alignment.astype(jnp.float32) + merged).astype(jnp.bfloat16)
    triangle_norm = normalize(triangle_local, 0).astype(jnp.bfloat16)
    update = project(triangle_norm, update_out_weight, "eij,ec->ijc") * update_gate
    pair_out = (pair_state + update).astype(jnp.bfloat16)
    return (alignment_out, pair_out)


def solution(mesh):
    placed = (
        P("dap", None, None),
        P("dap", None),
        P(),
        P(),
        P("dap", "hc", None),
        P(),
        P(),
        P(None, "hc"),
        P(None, "hc"),
        P(None, "hc"),
        P(None, "hc"),
        P(),
        P(),
        P(),
        P(),
        P(),
        P(),
        P(),
    )
    return jax.shard_map(
        on_device,
        mesh=mesh,
        in_specs=placed,
        out_specs=(P("dap", None, None), P("dap", "hc", None)),
        check_vma=False,
    )
```
